32 devices in a mesh: grp: 4 (over x, core), seq: 8 (over z, y).
Axes of the slice: x: 2, y: 2, z: 4, core: 2. Of those that a mesh axis runs over, the one named last changes fastest.
Arguments:
- patches: bfloat16 [2048, 1280], P(('grp', 'seq')), may hold values from -60 to 60
- piece_ids: int32 [32, 64], P(('grp', 'seq')), may hold values from 0 to 2, never falling along the last dimension, each value on 1 to 48 neighbouring positions
- vit_gain: float32 [1280], replicated, may hold values from 0.25 to 1.75
- vit_qkv: bfloat16 [1280, 3840], replicated
- vit_out: bfloat16 [1280, 1280], replicated, may hold values from -0.15625 to 0.15625
- merge_gain: float32 [1280], replicated, may hold values from 0.25 to 1.75
- merge_up: bfloat16 [5120, 5120], P(None, 'seq'), may hold values from -0.078125 to 0.078125
- merge_down: bfloat16 [5120, 8192], P(None, 'seq'), may hold values from -0.078125 to 0.078125
- dest: int32 [512], P(('grp', 'seq')), may hold values from 0 to 7, as said below
- tokens: bfloat16 [8192, 8192], P(('grp', 'seq')), may hold values from -60 to 60
- image_index: int32 [8192], P(('grp', 'seq')), may hold values from 0 to 32, as said below
- doc_lengths: int32 [4, 4], P('grp'), may hold values from 1 to 1024, 2048 in all within a row
- attn_gain: float32 [8192], replicated, may hold values from 0.25 to 1.75
- attn_qkv: bfloat16 [8192, 768], P(('grp', 'seq'))
- attn_out: bfloat16 [512, 8192], P(None, ('grp', 'seq')), may hold values from -0.25 to 0.25
Outputs:
- layer_out: bfloat16 [8192, 8192], P(('grp', 'seq'))
The draws below stay inside these ranges and needn't reach their ends.
Inputs may be any that keep to these rules, and one draw needn't show every extreme that they name: `dest`: within each aligned block of 16 rows (one device's merged rows), exactly 4 distinct values occur, each exactly 4 times, and in every group one device is named by every device of the group. `image_index`: 32 marks a text token. A value k < 32 on a device names the merged row that the device of seq index k // 4 in its group sends to it as its (k % 4)-th row in row order; each such row is named by exactly one token of the receiving device, and no other values occur. `piece_ids`: piece numbers never fall within a window. `doc_lengths`: each group's documents fill its 2048 positions.
All inputs are finite; a program needn't handle non-finite values.
Results may differ from the reference program's by a relative error of at most 0.0093.
The reference program's roundings to bfloat16 on the way count: a program that leaves them out, or rounds other values in their place, can miss the bound.
Values may be sent and summed in bfloat16 or wider, within the bound.
A program may use at most 192 MiB of HBM per device.

```python
import math
import jax
import jax.numpy as jnp
import numpy as np
from jax import lax

D = 8192
VD = 1280
VHEADS = 16
HEAD = 128
HQ = 4
WIN = 64
DOCS = 4
TOK_DEV = 256
M_DEV = 16
CAP = 4
SLOTS = 32
PATCHES = 2048
WINDOWS = 32
MERGED = 512
GROUP_TOK = 2048
TOKENS = 8192
MOST_DOC = 1024
N_GRP = 4
N_SEQ = 8


def scaled_field(key, row_count, col_count):
    parts = jax.random.split(key, 3)
    row_scale = jnp.exp(jax.random.uniform(parts[1], (row_count, 1), jnp.float32, jnp.log(0.3), jnp.log(3.0)))
    col_scale = jnp.exp(jax.random.uniform(parts[2], (1, col_count), jnp.float32, jnp.log(0.3), jnp.log(3.0)))
    base = jnp.clip(jax.random.normal(parts[0], (row_count, col_count), jnp.float32), -6.0, 6.0)
    return base * row_scale * col_scale


def draw_patches(key, part):
    return scaled_field(jax.random.fold_in(key, 11), PATCHES, VD).astype(jnp.bfloat16)


def draw_tokens(key, part):
    return scaled_field(jax.random.fold_in(key, 12), TOKENS, D).astype(jnp.bfloat16)


def draw_vit_qkv(key, part):
    parts = jax.random.split(jax.random.fold_in(key, 13), 1)
    base = jnp.clip(jax.random.normal(parts[0], (VD, 3 * VD), jnp.float32), -6.0, 6.0) * VD ** (-0.5)
    return base.astype(jnp.bfloat16)


def draw_attn_qkv(key, part):
    parts = jax.random.split(jax.random.fold_in(key, 14), 1)
    base = jnp.clip(jax.random.normal(parts[0], (D, (HQ + 2) * HEAD), jnp.float32), -6.0, 6.0) * D ** (-0.5)
    return base.astype(jnp.bfloat16)


def route_tables(key):
    base_key = jax.random.fold_in(key, 5)
    fanout = N_SEQ // 2
    sequence_ids = jnp.arange(N_SEQ, dtype=jnp.int32)
    row_ids = jnp.arange(M_DEV, dtype=jnp.int32)
    slot_ids = jnp.arange(CAP, dtype=jnp.int32)

    def one_group(group_key):
        parts = jax.random.split(group_key, 4)
        preference_boost = jax.random.permutation(parts[0], N_SEQ).astype(jnp.int32)
        random_jitter = jax.random.randint(parts[1], (N_SEQ, N_SEQ), 0, 1 << 20, dtype=jnp.int32)
        extra_reward = jnp.where(preference_boost == 0, 1 << 22, (N_SEQ - preference_boost) * (1 << 14)).astype(jnp.int32)
        score_value = (random_jitter + extra_reward[None, :]) * N_SEQ + sequence_ids[None, :]
        chosen = lax.top_k(score_value, fanout)[1].astype(jnp.int32)
        shuffles = jax.vmap(lambda shuffle_key: jax.random.permutation(shuffle_key, M_DEV))(jax.random.split(parts[2], N_SEQ)).astype(jnp.int32)
        targets = jnp.take_along_axis(chosen, shuffles // CAP, axis=1)
        same = targets[:, :, None] == targets[:, None, :]
        earlier = row_ids[None, :] < row_ids[:, None]
        order = jnp.sum(same & earlier[None], axis=-1).astype(jnp.int32)
        match = (targets[None, :, None, :] == sequence_ids[:, None, None, None]) & (order[None, :, None, :] == slot_ids[None, None, :, None])
        filled = jnp.any(match, axis=-1).reshape(N_SEQ, SLOTS)
        places = jax.vmap(lambda place_key: jax.random.permutation(place_key, TOK_DEV)[:SLOTS])(jax.random.split(parts[3], N_SEQ)).astype(jnp.int32)
        token_ids = jnp.arange(TOK_DEV, dtype=jnp.int32)
        hit = (places[:, :, None] == token_ids[None, None, :]) & filled[:, :, None]
        slot_all = jnp.arange(SLOTS, dtype=jnp.int32)
        named = jnp.sum(jnp.where(hit, slot_all[None, :, None], 0), axis=1)
        index = named + jnp.where(jnp.any(hit, axis=1), 0, SLOTS)
        return (targets.reshape(-1), index.reshape(-1))
    targets_all, index_all = jax.vmap(one_group)(jax.random.split(base_key, N_GRP))
    return (targets_all.reshape(-1).astype(jnp.int32), index_all.reshape(-1).astype(jnp.int32))


def draw_dest(key, part):
    return route_tables(key)[0]


def draw_image_index(key, part):
    return route_tables(key)[1]


def block_scale(own_key, shape, pieces, low, top_value):
    loudness, own = 1.0, jax.random.fold_in(own_key, 6)
    for position, blocks in pieces:
        steps = jnp.exp(jax.random.uniform(jax.random.fold_in(own, position), (blocks,), jnp.float32, low / len(pieces), top_value / len(pieces)))
        loudness = loudness * jnp.repeat(steps, shape[position] // blocks).reshape([-1 if axis == position else 1 for axis in range(len(shape))])
    return loudness


def length_profile(count, total, bound, skew):
    weights = [(1 << 20) // math.isqrt(standing ** skew) + 1 for standing in range(2, count + 1)]
    surplus, holding = total - bound - (count - 1), [1] * (count - 1)
    while surplus > 0:
        candidates = [i for i in range(count - 1) if holding[i] < bound]
        pool, budget = sum([weights[i] for i in candidates]), surplus
        for i in candidates:
            addition = min(bound - holding[i], max(1, budget * weights[i] // pool), surplus)
            holding[i] = holding[i] + addition
            surplus = surplus - addition
    return np.array([bound] + holding)


def ragged_sizes(key, number_of, total, limit, lean):
    if number_of == 2:
        one = jax.random.randint(key, (), max(1, total - limit), min(limit, total - 1) + 1)
        return jnp.stack([one, total - one])
    sizes = jnp.asarray(length_profile(number_of, total, limit, lean), jnp.int32)
    couples = (number_of - 1) // 2
    giver, taker = sizes[1:1 + 2 * couples:2], sizes[2:2 + 2 * couples:2]
    room = jnp.minimum(giver - 1, limit - taker)
    shifted = jax.random.randint(jax.random.fold_in(key, 1), (couples,), 0, 1 << 20) % (room + 1)
    sizes = sizes.at[1:1 + 2 * couples:2].set(giver - shifted).at[2:2 + 2 * couples:2].set(taker + shifted)
    return sizes[jax.random.permutation(jax.random.fold_in(key, 2), number_of)]


def centred(own_key, shape, width, reach, cuts=(), held_as=jnp.bfloat16):
    level = block_scale(own_key, shape, cuts, -0.22, 0.18) if cuts else 1.0
    result = jax.random.normal(own_key, shape, jnp.float32) * width * level
    return jnp.minimum(jnp.maximum(result, -reach), reach).astype(held_as)


def setup_inputs(seed: int = 0) -> dict:
    key_list = jax.random.split(jax.random.key(seed), 16)
    patches = draw_patches(jax.random.fold_in(key_list[15], 71), 0)
    piece_ids = jax.vmap(lambda own: jnp.searchsorted(jnp.cumsum(ragged_sizes(own, 3, WIN, 48, 2)), jnp.arange(WIN), side="right"))(jax.random.split(key_list[1], WINDOWS)).reshape((WINDOWS, WIN)).astype(jnp.int32)
    vit_gain = jnp.clip(1.0 + 0.15 * jax.random.normal(key_list[2], (VD,), jnp.float32), 0.25, 1.75)
    vit_qkv = draw_vit_qkv(jax.random.fold_in(key_list[15], 71), 0)
    vit_out = centred(key_list[4], (VD, VD), VD ** -0.5, 0.15625)
    merge_gain = jnp.clip(1.0 + 0.15 * jax.random.normal(key_list[5], (VD,), jnp.float32), 0.25, 1.75)
    merge_up = centred(key_list[6], (4 * VD, 4 * VD), (4 * VD) ** -0.5, 0.078125, ((1, 8),))
    merge_down = centred(key_list[7], (4 * VD, D), (4 * VD) ** -0.5, 0.078125, ((1, 8),))
    dest = draw_dest(jax.random.fold_in(key_list[15], 71), 0)
    tokens = draw_tokens(jax.random.fold_in(key_list[15], 71), 0)
    image_index = draw_image_index(jax.random.fold_in(key_list[15], 71), 0)
    doc_lengths = jax.vmap(lambda own: ragged_sizes(own, DOCS, GROUP_TOK, MOST_DOC, 2))(jax.random.split(key_list[11], N_GRP)).reshape((N_GRP, DOCS)).astype(jnp.int32)
    attn_gain = jnp.clip(1.0 + 0.15 * jax.random.normal(key_list[12], (D,), jnp.float32), 0.25, 1.75)
    attn_qkv = draw_attn_qkv(jax.random.fold_in(key_list[15], 71), 0)
    attn_out = centred(key_list[14], (HQ * HEAD, D), (HQ * HEAD) ** -0.5, 0.25, ((1, 32),))
    return dict(patches=patches, piece_ids=piece_ids, vit_gain=vit_gain, vit_qkv=vit_qkv, vit_out=vit_out, merge_gain=merge_gain, merge_up=merge_up, merge_down=merge_down, dest=dest, tokens=tokens, image_index=image_index, doc_lengths=doc_lengths, attn_gain=attn_gain, attn_qkv=attn_qkv, attn_out=attn_out)


EPSILON = 1e-06

def rms_scale(inputs, gain):
    mean_square = lax.optimization_barrier(jnp.mean(inputs * inputs, axis=-1, keepdims=True))
    return inputs * lax.rsqrt(mean_square + EPSILON) * gain

def softmax_mix(scores, allowed, value_collection, spec):
    scores = jnp.where(allowed[None], scores, -1e+30)
    highest = lax.optimization_barrier(jnp.max(scores, axis=-1, keepdims=True))
    weights = jnp.exp(scores - highest)
    totals = lax.optimization_barrier(jnp.sum(weights, axis=-1))
    rounded_values = lax.optimization_barrier(weights.astype(jnp.bfloat16)).astype(jnp.float32)
    mixture = jnp.einsum(spec, rounded_values, value_collection.astype(jnp.float32))
    return mixture / jnp.transpose(totals)[:, :, None]

def window_layer(patch_rows, piece_rows, vit_gain, vit_qkv, vit_out, merge_gain):
    row_count, features = patch_rows.shape
    head_dim = features // VHEADS
    residual = patch_rows.astype(jnp.float32)
    normed = rms_scale(residual, vit_gain).astype(jnp.bfloat16)
    projected = jnp.dot(normed, vit_qkv, preferred_element_type=jnp.float32).astype(jnp.bfloat16)
    queries = projected[:, :features].reshape(row_count, VHEADS, head_dim)
    key_set = projected[:, features:2 * features].reshape(row_count, VHEADS, head_dim)
    value_collection = projected[:, 2 * features:].reshape(row_count, VHEADS, head_dim)
    scores = jnp.einsum('qhd,khd->hqk', queries.astype(jnp.float32), key_set.astype(jnp.float32)) * head_dim ** (-0.5)
    frames = jnp.arange(row_count, dtype=jnp.int32) // WIN
    allowed = (frames[:, None] == frames[None, :]) & (piece_rows[:, None] == piece_rows[None, :])
    mixture = softmax_mix(scores, allowed, value_collection, 'hqk,khd->qhd')
    mixture = mixture.reshape(row_count, features).astype(jnp.bfloat16)
    residual = residual + jnp.dot(mixture, vit_out, preferred_element_type=jnp.float32)
    merge_input = rms_scale(residual, merge_gain).astype(jnp.bfloat16)
    return merge_input.reshape(row_count // 4, 4 * features)

def attend(query_rows, query_pos, query_start, key_value, key_pos):
    row_count = query_rows.shape[0]
    head_dim = key_value.shape[1] // 2
    heads = query_rows.shape[1] // head_dim
    queries = query_rows.reshape(row_count, heads, head_dim)
    scores = jnp.einsum('qhd,kd->hqk', queries.astype(jnp.float32), key_value[:, :head_dim].astype(jnp.float32)) * head_dim ** (-0.5)
    allowed = (key_pos[None, :] >= query_start[:, None]) & (key_pos[None, :] <= query_pos[:, None])
    mixture = softmax_mix(scores, allowed, key_value[:, head_dim:], 'hqk,kd->qhd')
    return mixture.reshape(row_count, heads * head_dim).astype(jnp.bfloat16)

def slot_numbers(targets):
    row_count = targets.shape[-1]
    order = jnp.arange(row_count, dtype=jnp.int32)
    same = targets[..., :, None] == targets[..., None, :]
    earlier = order[None, :] < order[:, None]
    return lax.optimization_barrier(jnp.sum(same & earlier, axis=-1)).astype(jnp.int32)

def prefill_group(layer_in, lengths, attn_gain, attn_qkv, attn_out):
    normed = rms_scale(layer_in.astype(jnp.float32), attn_gain).astype(jnp.bfloat16)
    projected = jnp.dot(normed, attn_qkv, preferred_element_type=jnp.float32).astype(jnp.bfloat16)
    query_width = HQ * HEAD
    queries = projected[:, :query_width]
    key_value = projected[:, query_width:]
    positions = jnp.arange(GROUP_TOK, dtype=jnp.int32)
    starts = (jnp.cumsum(lengths) - lengths).astype(jnp.int32)
    doc_start = lax.optimization_barrier(jnp.max(jnp.where(starts[None, :] <= positions[:, None], starts[None, :], 0), axis=1)).astype(jnp.int32)
    block_rows = min(GROUP_TOK, 512)
    attended = lax.map(lambda parts: attend(parts[0], parts[1], parts[2], key_value, positions), (queries.reshape(-1, block_rows, query_width), positions.reshape(-1, block_rows), doc_start.reshape(-1, block_rows))).reshape(GROUP_TOK, query_width)
    update = jnp.dot(attended, attn_out, preferred_element_type=jnp.float32)
    return (layer_in.astype(jnp.float32) + update).astype(jnp.bfloat16)

def reference(patches, piece_ids, vit_gain, vit_qkv, vit_out, merge_gain, merge_up, merge_down, dest, tokens, image_index, doc_lengths, attn_gain, attn_qkv, attn_out):
    block_len = WIN
    patch_blocks = patches.reshape(PATCHES // block_len, block_len, VD)
    piece_blocks = piece_ids.reshape(PATCHES // block_len, block_len)
    merge_input = lax.map(lambda parts: window_layer(parts[0], parts[1], vit_gain, vit_qkv, vit_out, merge_gain), (patch_blocks, piece_blocks)).reshape(MERGED, 4 * VD)
    hidden = jax.nn.gelu(jnp.dot(merge_input, merge_up, preferred_element_type=jnp.float32), approximate=False).astype(jnp.bfloat16)
    merged_rows = jnp.dot(hidden, merge_down, preferred_element_type=jnp.float32).astype(jnp.bfloat16)
    merged_rows = merged_rows.reshape(N_GRP, N_SEQ, M_DEV, D)
    targets = dest.reshape(N_GRP, N_SEQ, M_DEV)
    orders = slot_numbers(targets)
    receivers = jnp.arange(N_SEQ, dtype=jnp.int32)
    row_ids = jnp.arange(M_DEV, dtype=jnp.int32)
    slot_ids = jnp.arange(CAP, dtype=jnp.int32)
    index_all = image_index.reshape(N_GRP, N_SEQ, TOK_DEV)
    token_all = tokens.reshape(N_GRP, N_SEQ, TOK_DEV, D)
    results = []
    for group in range(N_GRP):
        match = (targets[group][None, :, None, :] == receivers[:, None, None, None]) & (orders[group][None, :, None, :] == slot_ids[None, None, :, None])
        row_pick = lax.optimization_barrier(jnp.sum(jnp.where(match, row_ids, 0), axis=-1)).astype(jnp.int32)
        source_list = jnp.broadcast_to(receivers[None, :, None], row_pick.shape)
        table = merged_rows[group][source_list, row_pick].reshape(N_SEQ, SLOTS, D)
        index_rows = index_all[group]
        picked = jax.vmap(lambda table_rows, wanted: table_rows[jnp.minimum(wanted, SLOTS - 1)])(table, index_rows)
        layer_in = jnp.where((index_rows < SLOTS)[:, :, None], picked, token_all[group]).reshape(GROUP_TOK, D)
        results.append(prefill_group(layer_in, doc_lengths[group], attn_gain, attn_qkv, attn_out))
    return jnp.concatenate(results, axis=0)
```

```python
import functools

import jax
import jax.numpy as jnp
from jax import lax
from jax.experimental import pallas as pl
from jax.experimental.pallas import tpu as pltpu
from jax.sharding import PartitionSpec as P

VHEADS = 16
WIN = 64
LANES = 128
EPSILON = 1e-06
MESH = pl.DeviceIdType.MESH


def rms_scale(inputs, gain):
    mean_square = jnp.mean(inputs * inputs, axis=-1, keepdims=True)
    return inputs * lax.rsqrt(mean_square + EPSILON) * gain


def slot_numbers(targets):
    row_count = targets.shape[-1]
    order = jnp.arange(row_count, dtype=jnp.int32)
    same = targets[..., :, None] == targets[..., None, :]
    earlier = order[None, :] < order[:, None]
    return jnp.sum(same & earlier, axis=-1)


def greet(n_seq, pairs):
    grp, seq = lax.axis_index("grp"), lax.axis_index("seq")
    barrier = pltpu.get_barrier_semaphore()
    for k in range(1, n_seq):
        pl.semaphore_signal(
            barrier, inc=1, device_id=(grp, lax.rem(seq + k, n_seq)), device_id_type=MESH
        )
    for other in pairs:
        pl.semaphore_signal(barrier, inc=1, device_id=(other, seq), device_id_type=MESH)
    pl.semaphore_wait(barrier, n_seq - 1 + len(pairs))


def flip(index, bit):
    return index + bit - 2 * bit * lax.rem(index // bit, 2)


class Relay:
    def __init__(self, n_seq, shard, full, local_sem, recv_sem, send_sem):
        self.n_seq, self.shard, self.full = n_seq, shard, full
        self.local_sem, self.recv_sem, self.send_sem = local_sem, recv_sem, send_sem
        self.line = n_seq // 2
        self.grp, self.seq = lax.axis_index("grp"), lax.axis_index("seq")
        self.core = lax.rem(self.grp, 2)
        self.place, self.side = self.seq // 2, lax.rem(self.seq, 2)
        far = flip(self.grp, 2)
        self.far = far
        across = flip(self.seq, 1)
        first = self.core == 0
        self.a_dev = (jnp.where(first, far, self.grp), jnp.where(first, self.seq, across))
        self.b_dev = (jnp.where(first, self.grp, far), jnp.where(first, across, self.seq))
        self.ab_dev = (far, across)
        self.core_dev = (flip(self.grp, 1), self.seq)

    def slot(self, base, place):
        return base[0] * self.n_seq + 2 * place + lax.rem(base[1], 2)

    def copy(self, slot, way, device, own=False):
        return pltpu.make_async_remote_copy(
            src_ref=self.shard if own else self.full.at[slot],
            dst_ref=self.full.at[slot],
            send_sem=self.send_sem.at[way, slot],
            recv_sem=self.recv_sem.at[slot],
            device_id=device,
            device_id_type=MESH,
        )

    def up(self):
        return (self.grp, jnp.minimum(self.seq + 2, self.n_seq - 2 + self.side))

    def down(self):
        return (self.grp, jnp.maximum(self.seq - 2, self.side))

    def me(self):
        return (self.grp, self.seq)

    def begin(self):
        slot = self.slot(self.me(), self.place)
        pltpu.make_async_copy(self.shard, self.full.at[slot], self.local_sem).start()

        @pl.when(self.place + 1 < self.line)
        def _():
            self.copy(slot, 0, self.up(), True).start()

        @pl.when(self.place > 0)
        def _():
            self.copy(slot, 1, self.down(), True).start()

        self.copy(slot, 2, self.a_dev, True).start()
        self.copy(slot, 3, self.b_dev, True).start()
        self.copy(slot, 4, self.core_dev, True).start()

    def spots(self, distance):
        low, high = self.place - distance, self.place + distance
        if distance == 0:
            return [(self.place, None, None)]
        return [(low, low >= 0, True), (high, high < self.line, False)]

    def visit(self, base, distance, ways, finish=False):
        for place, there, upward in self.spots(distance):

            def act(place=place, upward=upward):
                slot = self.slot(base, place)
                own_core = base is not None
                if not finish:
                    self.copy(slot, 4, self.core_dev).wait_recv()
                for way, device in ways:
                    move = self.copy(slot, way, device)
                    move.wait_send() if finish else move.start()
                if upward is True and "z" in self.mode:

                    @pl.when(self.place + 1 < self.line)
                    def _():
                        move = self.copy(slot, 0, self.up())
                        move.wait_send() if finish else move.start()

                if upward is False and "z" in self.mode:

                    @pl.when(self.place > 0)
                    def _():
                        move = self.copy(slot, 1, self.down())
                        move.wait_send() if finish else move.start()

            if there is None:
                act()
            else:
                pl.when(there)(act)

    def own_line(self, distance, finish=False):
        self.mode = "z"
        self.visit(
            self.me(), distance,
            [(2, self.a_dev), (3, self.b_dev), (4, self.core_dev)], finish,
        )

    def a_line(self, distance, finish=False):
        self.mode = ""
        self.visit(self.a_dev, distance, [(3, self.b_dev), (4, self.core_dev)], finish)

    def b_lines(self, distance, finish=False):
        self.mode = ""
        self.visit(self.b_dev, distance, [(4, self.core_dev)], finish)
        self.visit(self.ab_dev, distance, [(4, self.core_dev)], finish)

    def step(self, distance):
        if 0 < distance < self.line:
            self.own_line(distance)
        if 0 <= distance - 1 < self.line:
            self.a_line(distance - 1)
        if 0 <= distance - 2 < self.line:
            self.b_lines(distance - 2)

    def steps(self):
        return self.line + 2

    def end(self):
        slot = self.slot(self.me(), self.place)
        pltpu.make_async_copy(self.shard, self.full.at[slot], self.local_sem).wait()

        @pl.when(self.place + 1 < self.line)
        def _():
            self.copy(slot, 0, self.up(), True).wait_send()

        @pl.when(self.place > 0)
        def _():
            self.copy(slot, 1, self.down(), True).wait_send()

        self.copy(slot, 2, self.a_dev, True).wait_send()
        self.copy(slot, 3, self.b_dev, True).wait_send()
        self.copy(slot, 4, self.core_dev, True).wait_send()
        for distance in range(self.line):
            if distance:
                self.own_line(distance, True)
            self.a_line(distance, True)
            self.b_lines(distance, True)
        partner = self.core_dev[0]
        for place in range(self.line):
            for base in (
                (partner, self.seq), (partner, flip(self.seq, 1)),
                (flip(partner, 2), self.seq), (flip(partner, 2), flip(self.seq, 1)),
            ):
                slot = self.slot(base, place)
                self.copy(slot, 4, self.core_dev).wait_recv()


def relay_scratch(n_dev):
    return [
        pltpu.SemaphoreType.DMA,
        pltpu.SemaphoreType.DMA((n_dev,)),
        pltpu.SemaphoreType.DMA((5, n_dev)),
    ]


def swap(n_seq, send_of, land_of, send_sem, recv_sem):
    grp, seq = lax.axis_index("grp"), lax.axis_index("seq")
    moves = []
    for k in range(1, n_seq):
        to = lax.rem(seq + k, n_seq)
        moves.append(
            pltpu.make_async_remote_copy(
                src_ref=send_of(to),
                dst_ref=land_of(seq),
                send_sem=send_sem.at[k],
                recv_sem=recv_sem.at[k],
                device_id=(grp, to),
                device_id_type=MESH,
            )
        )
    for move in moves:
        move.start()
    return moves


def vision_kernel(
    n_seq, slots,
    patches, piece_col, piece_row, vit_gain, vit_qkv, vit_out, merge_gain, merge_up, merge_down,
    code, want, row_base, attn_qkv,
    table, qkv_all,
    up_v, down_v, normed_s, gathered, hidden, stage, landed,
    load_sem, send1, recv1, send2, recv2, send3, recv3, *relay_sems,
):
    seq = lax.axis_index("seq")
    grp = lax.axis_index("grp")
    up_copy = pltpu.make_async_copy(merge_up, up_v, load_sem.at[0])
    down_copy = pltpu.make_async_copy(merge_down, down_v, load_sem.at[1])
    up_copy.start()
    down_copy.start()
    greet(n_seq, (flip(grp, 1), flip(grp, 2)))
    relay = Relay(n_seq, attn_qkv, qkv_all, *relay_sems)
    relay.begin()

    rows, features = patches.shape
    head_dim = features // VHEADS
    residual = patches[...].astype(jnp.float32)
    normed = rms_scale(residual, vit_gain[...]).astype(jnp.bfloat16)
    projected = jnp.dot(normed, vit_qkv[...], preferred_element_type=jnp.float32)
    q = projected[:, :features].astype(jnp.bfloat16).astype(jnp.float32)
    keys = projected[:, features : 2 * features].astype(jnp.bfloat16)
    values = projected[:, 2 * features :].astype(jnp.bfloat16)
    lane = lax.broadcasted_iota(jnp.int32, (rows, features), 1)
    inside = [(lane >= h * head_dim) & (lane < (h + 1) * head_dim) for h in range(VHEADS)]
    stacked = jnp.concatenate(
        [jnp.where(inside[h], q, 0.0).astype(jnp.bfloat16) for h in range(VHEADS)], axis=0
    )
    scores = lax.dot_general(
        stacked, keys, (((1,), (1,)), ((), ())), preferred_element_type=jnp.float32
    ) * head_dim ** (-0.5)
    scores = scores.reshape(VHEADS, rows, rows)
    allowed = piece_col[...] == piece_row[...]
    scores = jnp.where(allowed[None], scores, -1e30)
    weights = jnp.exp(scores - jnp.max(scores, axis=-1, keepdims=True))
    totals = jnp.sum(weights, axis=-1, keepdims=True)
    mixed = jnp.dot(
        weights.reshape(VHEADS * rows, rows).astype(jnp.bfloat16), values,
        preferred_element_type=jnp.float32,
    )
    top = jnp.zeros((rows, features), jnp.float32)
    low = jnp.ones((rows, features), jnp.float32)
    for h in range(VHEADS):
        top = jnp.where(inside[h], mixed[h * rows : (h + 1) * rows], top)
        low = jnp.where(inside[h], totals[h], low)
    mixture = (top / low).astype(jnp.bfloat16)
    residual = residual + jnp.dot(mixture, vit_out[...], preferred_element_type=jnp.float32)
    merged_in = rms_scale(residual, merge_gain[...])
    own = rows // 4
    chunks = features // LANES
    for j in range(chunks):
        normed_s[j] = merged_in[:, j * LANES : (j + 1) * LANES]
    for part in range(4):
        for j in range(chunks):
            start = part * features + j * LANES
            gathered[seq, :, start : start + LANES] = normed_s[
                j, pl.ds(part, own, stride=4), :
            ].astype(jnp.bfloat16)
    gathered[seq, :, 4 * features :] = code[...]
    moves1 = swap(n_seq, lambda to: gathered.at[seq], lambda me: gathered.at[me], send1, recv1)
    up_copy.wait()
    for move in moves1:
        move.wait_recv()
    all_rows = n_seq * own
    entry = gathered[:, :, : 4 * features].reshape(all_rows, 4 * features)
    pre = jnp.dot(entry, up_v[...], preferred_element_type=jnp.float32)
    hidden[seq] = (0.5 * pre * (1.0 + lax.erf(pre * 0.5**0.5))).astype(jnp.bfloat16)
    moves2 = swap(n_seq, lambda to: hidden.at[seq], lambda me: hidden.at[me], send2, recv2)
    down_copy.wait()
    part_width = hidden.shape[2]

    def term(source):
        start = pl.multiple_of(source * part_width, 32)
        return jnp.dot(
            hidden[source], down_v[pl.ds(start, part_width), :], preferred_element_type=jnp.float32
        )

    codes = gathered[:, :, 4 * features :].reshape(all_rows, LANES).astype(jnp.float32)[:, :1]
    select = jnp.where(codes + row_base[...] == want[...], 1.0, 0.0)
    select = jnp.transpose(select).astype(jnp.bfloat16)
    total = term(seq)
    for k in range(1, n_seq):
        moves2[k - 1].wait_recv()
        total = total + term(lax.rem(seq - k + n_seq, n_seq))
    outgoing = jnp.dot(
        select, total.astype(jnp.bfloat16), preferred_element_type=jnp.float32
    ).astype(jnp.bfloat16)
    stage[...] = outgoing.reshape(stage.shape)
    landed[seq] = stage[seq]
    moves3 = swap(n_seq, lambda to: stage.at[to], lambda me: landed.at[me], send3, recv3)
    for distance in range(relay.steps()):
        relay.step(distance)
    for move in moves3:
        move.wait_recv()
    width = landed.shape[2]
    for source in range(n_seq):
        table[:, source * width : (source + 1) * width] = landed[source]
    for moves in (moves1, moves2, moves3):
        for move in moves:
            move.wait_send()
    relay.end()


def attend_kernel(
    n_seq, reach, heads,
    queries, own_kv, positions, starts, attn_out,
    attended, out_all,
    kv, load_sem, send_sem, recv_sem, *relay_sems,
):
    grp, seq = lax.axis_index("grp"), lax.axis_index("seq")
    rows, width = own_kv.shape
    head_dim = width // 2
    greet(n_seq, (flip(grp, 1), flip(grp, 2)))
    moves = []
    for k in range(1, reach + 1):
        moves.append(
            pltpu.make_async_remote_copy(
                src_ref=own_kv,
                dst_ref=kv.at[reach - k],
                send_sem=send_sem.at[k],
                recv_sem=recv_sem.at[k],
                device_id=(grp, lax.rem(seq + k, n_seq)),
                device_id_type=MESH,
            )
        )
    for move in moves:
        move.start()
    relay = Relay(n_seq, attn_out, out_all, *relay_sems)
    relay.begin()
    kv[reach] = own_kv[...]
    for move in moves:
        move.wait_recv()
    span = (reach + 1) * rows
    everything = kv[...].reshape(span, width)
    keys, values = everything[:, :head_dim], everything[:, head_dim:]
    key_pos = (seq - reach) * rows + lax.broadcasted_iota(jnp.int32, (rows, span), 1)
    allowed = (key_pos >= starts[...]) & (key_pos <= positions[...])
    for distance in range(relay.steps()):
        relay.step(distance)
        for h in range(heads) if distance == 1 else ():
            scores = lax.dot_general(
                queries[:, h * head_dim : (h + 1) * head_dim], keys,
                (((1,), (1,)), ((), ())), preferred_element_type=jnp.float32,
            ) * head_dim ** (-0.5)
            scores = jnp.where(allowed, scores, -1e30)
            weights = jnp.exp(scores - jnp.max(scores, axis=-1, keepdims=True))
            totals = jnp.sum(weights, axis=-1, keepdims=True)
            mixed = jnp.dot(
                weights.astype(jnp.bfloat16), values, preferred_element_type=jnp.float32
            )
            attended[:, h * head_dim : (h + 1) * head_dim] = (mixed / totals).astype(jnp.bfloat16)
    for move in moves:
        move.wait_send()
    relay.end()


def out_kernel(attended, weight, layer_in, result):
    width = weight.shape[2]
    for i in range(weight.shape[0]):
        columns = slice(i * width, (i + 1) * width)
        update = jnp.dot(attended[...], weight[i], preferred_element_type=jnp.float32)
        result[:, columns] = (layer_in[:, columns].astype(jnp.float32) + update).astype(jnp.bfloat16)


VMEM = pl.BlockSpec(memory_space=pltpu.VMEM)
ANY = pl.BlockSpec(memory_space=pl.ANY)


def on_device(
    patches, piece_ids, vit_gain, vit_qkv, vit_out, merge_gain, merge_up, merge_down, dest,
    tokens, image_index, doc_lengths, attn_gain, attn_qkv, attn_out,
):
    rows, features = patches.shape
    n_seq, n_grp = lax.axis_size("seq"), lax.axis_size("grp")
    n_dev = n_seq * n_grp
    seq_index = lax.axis_index("seq")
    own = rows // 4
    all_rows = n_seq * own
    capacity = own // (n_seq // 2)
    slots = n_seq * capacity
    bf16, f32 = jnp.bfloat16, jnp.float32

    windows = jnp.arange(rows, dtype=jnp.int32) // WIN
    pieces = piece_ids.reshape(-1) + windows * WIN
    code = dest * capacity + slot_numbers(dest).astype(jnp.int32)
    code = jnp.broadcast_to(code[:, None], (own, LANES)).astype(bf16)
    column = jnp.arange(n_seq * slots, dtype=jnp.int32)
    target, place = column // slots, column % slots
    want = (place // capacity) * (n_seq * capacity) + target * capacity + place % capacity
    row_base = (jnp.arange(all_rows, dtype=jnp.int32) // own) * (n_seq * capacity)

    up_width, down_width = merge_up.shape[1], merge_down.shape[1]
    table, qkv_all = pl.pallas_call(
        functools.partial(vision_kernel, n_seq, slots),
        out_shape=(
            jax.ShapeDtypeStruct((slots, n_seq * down_width), bf16),
            jax.ShapeDtypeStruct((n_dev,) + attn_qkv.shape, bf16),
        ),
        in_specs=[VMEM] * 7 + [ANY] * 2 + [VMEM] * 3 + [ANY],
        out_specs=(VMEM, ANY),
        scratch_shapes=[
            pltpu.VMEM(merge_up.shape, bf16),
            pltpu.VMEM(merge_down.shape, bf16),
            pltpu.VMEM((features // LANES, rows, LANES), f32),
            pltpu.VMEM((n_seq, own, 4 * features + LANES), bf16),
            pltpu.VMEM((n_seq, all_rows, up_width), bf16),
            pltpu.VMEM((n_seq, slots, down_width), bf16),
            pltpu.VMEM((n_seq, slots, down_width), bf16),
            pltpu.SemaphoreType.DMA((2,)),
        ] + [pltpu.SemaphoreType.DMA((n_seq,))] * 6 + relay_scratch(n_dev),
        compiler_params=pltpu.CompilerParams(
            collective_id=0, has_side_effects=True, vmem_limit_bytes=66000000
        ),
    )(
        patches, pieces[:, None], pieces[None, :], vit_gain[None], vit_qkv, vit_out,
        merge_gain[None], merge_up, merge_down, code, want.astype(f32)[None],
        row_base.astype(f32)[:, None], attn_qkv,
    )

    slot_all = jnp.arange(slots, dtype=jnp.int32)
    picker = (image_index[:, None] == slot_all[None, :]).astype(bf16)
    pictured = jnp.dot(picker, table, preferred_element_type=f32).astype(bf16)
    layer_in = jnp.where((image_index < slots)[:, None], pictured, tokens)
    tok_rows = tokens.shape[0]
    normed = rms_scale(layer_in.astype(f32), attn_gain).astype(bf16)
    projected = jnp.dot(
        normed, qkv_all.reshape(-1, attn_qkv.shape[1]), preferred_element_type=f32
    ).astype(bf16)
    query_width = attn_out.shape[0]
    queries = projected[:, :query_width]
    key_value = projected[:, query_width:]
    head_dim = key_value.shape[1] // 2
    head_count = query_width // head_dim
    positions = seq_index * tok_rows + jnp.arange(tok_rows, dtype=jnp.int32)
    lengths = doc_lengths[0]
    starts = jnp.cumsum(lengths) - lengths
    doc_start = jnp.max(
        jnp.where(starts[None, :] <= positions[:, None], starts[None, :], 0), axis=1
    )
    reach = n_seq // 2
    attended, out_all = pl.pallas_call(
        functools.partial(attend_kernel, n_seq, reach, head_count),
        out_shape=(
            jax.ShapeDtypeStruct((tok_rows, query_width), bf16),
            jax.ShapeDtypeStruct((n_dev,) + attn_out.shape, bf16),
        ),
        in_specs=[VMEM] * 4 + [ANY],
        out_specs=(VMEM, ANY),
        scratch_shapes=[
            pltpu.VMEM((reach + 1, tok_rows, 2 * head_dim), bf16),
            pltpu.SemaphoreType.DMA((2,)),
            pltpu.SemaphoreType.DMA((reach + 1,)),
            pltpu.SemaphoreType.DMA((reach + 1,)),
        ] + relay_scratch(n_dev),
        compiler_params=pltpu.CompilerParams(
            collective_id=1, has_side_effects=True, vmem_limit_bytes=60000000
        ),
    )(queries, key_value, positions[:, None], doc_start[:, None], attn_out)

    step = n_dev // 8
    wide = step * attn_out.shape[1]
    return pl.pallas_call(
        out_kernel,
        grid=(n_dev // step,),
        out_shape=jax.ShapeDtypeStruct(tokens.shape, bf16),
        in_specs=[
            pl.BlockSpec((tok_rows, query_width), lambda i: (0, 0)),
            pl.BlockSpec((step,) + attn_out.shape, lambda i: (i, 0, 0)),
            pl.BlockSpec((tok_rows, wide), lambda i: (0, i)),
        ],
        out_specs=pl.BlockSpec((tok_rows, wide), lambda i: (0, i)),
    )(attended, out_all, layer_in)


def solution(mesh):
    placed = (
        P(("grp", "seq"), None),
        P(("grp", "seq"), None),
        P(),
        P(),
        P(),
        P(),
        P(None, "seq"),
        P(None, "seq"),
        P(("grp", "seq")),
        P(("grp", "seq"), None),
        P(("grp", "seq")),
        P("grp", None),
        P(),
        P(("grp", "seq"), None),
        P(None, ("grp", "seq")),
    )
    return jax.shard_map(
        on_device, mesh=mesh, in_specs=placed, out_specs=P(("grp", "seq"), None), check_vma=False
    )
```

```python
import functools

import jax
import jax.numpy as jnp
from jax import lax
from jax.experimental import pallas as pl
from jax.experimental.pallas import tpu as pltpu
from jax.sharding import PartitionSpec as P

VHEADS = 16
WIN = 64
LANES = 128
EPSILON = 1e-06
MESH = pl.DeviceIdType.MESH


def rms_scale(inputs, gain):
    mean_square = jnp.mean(inputs * inputs, axis=-1, keepdims=True)
    return inputs * lax.rsqrt(mean_square + EPSILON) * gain


def slot_numbers(targets):
    row_count = targets.shape[-1]
    order = jnp.arange(row_count, dtype=jnp.int32)
    same = targets[..., :, None] == targets[..., None, :]
    earlier = order[None, :] < order[:, None]
    return jnp.sum(same & earlier, axis=-1)


def greet(n_seq, pairs):
    grp, seq = lax.axis_index("grp"), lax.axis_index("seq")
    barrier = pltpu.get_barrier_semaphore()
    for k in range(1, n_seq):
        pl.semaphore_signal(
            barrier, inc=1, device_id=(grp, lax.rem(seq + k, n_seq)), device_id_type=MESH
        )
    for other in pairs:
        pl.semaphore_signal(barrier, inc=1, device_id=(other, seq), device_id_type=MESH)
    pl.semaphore_wait(barrier, n_seq - 1 + len(pairs))


def flip(index, bit):
    return index + bit - 2 * bit * lax.rem(index // bit, 2)


class Relay:
    def __init__(self, n_seq, shard, full, local_sem, recv_sem, send_sem):
        self.n_seq, self.shard, self.full = n_seq, shard, full
        self.local_sem, self.recv_sem, self.send_sem = local_sem, recv_sem, send_sem
        self.line = n_seq // 2
        self.grp, self.seq = lax.axis_index("grp"), lax.axis_index("seq")
        self.core = lax.rem(self.grp, 2)
        self.place, self.side = self.seq // 2, lax.rem(self.seq, 2)
        far = flip(self.grp, 2)
        self.far = far
        across = flip(self.seq, 1)
        first = self.core == 0
        self.a_dev = (jnp.where(first, far, self.grp), jnp.where(first, self.seq, across))
        self.b_dev = (jnp.where(first, self.grp, far), jnp.where(first, across, self.seq))
        self.ab_dev = (far, across)
        self.core_dev = (flip(self.grp, 1), self.seq)

    def slot(self, base, place):
        return base[0] * self.n_seq + 2 * place + lax.rem(base[1], 2)

    def copy(self, slot, way, device, own=False):
        return pltpu.make_async_remote_copy(
            src_ref=self.shard if own else self.full.at[slot],
            dst_ref=self.full.at[slot],
            send_sem=self.send_sem.at[way, slot],
            recv_sem=self.recv_sem.at[slot],
            device_id=device,
            device_id_type=MESH,
        )

    def up(self):
        return (self.grp, jnp.minimum(self.seq + 2, self.n_seq - 2 + self.side))

    def down(self):
        return (self.grp, jnp.maximum(self.seq - 2, self.side))

    def me(self):
        return (self.grp, self.seq)

    def begin(self):
        slot = self.slot(self.me(), self.place)
        pltpu.make_async_copy(self.shard, self.full.at[slot], self.local_sem).start()

        @pl.when(self.place + 1 < self.line)
        def _():
            self.copy(slot, 0, self.up(), True).start()

        @pl.when(self.place > 0)
        def _():
            self.copy(slot, 1, self.down(), True).start()

        self.copy(slot, 2, self.a_dev, True).start()
        self.copy(slot, 3, self.b_dev, True).start()
        self.copy(slot, 4, self.core_dev, True).start()

    def spots(self, distance):
        low, high = self.place - distance, self.place + distance
        if distance == 0:
            return [(self.place, None, None)]
        return [(low, low >= 0, True), (high, high < self.line, False)]

    def visit(self, base, distance, ways, finish=False):
        for place, there, upward in self.spots(distance):

            def act(place=place, upward=upward):
                slot = self.slot(base, place)
                own_core = base is not None
                if not finish:
                    self.copy(slot, 4, self.core_dev).wait_recv()
                for way, device in ways:
                    move = self.copy(slot, way, device)
                    move.wait_send() if finish else move.start()
                if upward is True and "z" in self.mode:

                    @pl.when(self.place + 1 < self.line)
                    def _():
                        move = self.copy(slot, 0, self.up())
                        move.wait_send() if finish else move.start()

                if upward is False and "z" in self.mode:

                    @pl.when(self.place > 0)
                    def _():
                        move = self.copy(slot, 1, self.down())
                        move.wait_send() if finish else move.start()

            if there is None:
                act()
            else:
                pl.when(there)(act)

    def own_line(self, distance, finish=False):
        self.mode = "z"
        self.visit(
            self.me(), distance,
            [(2, self.a_dev), (3, self.b_dev), (4, self.core_dev)], finish,
        )

    def a_line(self, distance, finish=False):
        self.mode = ""
        self.visit(self.a_dev, distance, [(3, self.b_dev), (4, self.core_dev)], finish)

    def b_lines(self, distance, finish=False):
        self.mode = ""
        self.visit(self.b_dev, distance, [(4, self.core_dev)], finish)
        self.visit(self.ab_dev, distance, [(4, self.core_dev)], finish)

    def step(self, distance):
        if 0 < distance < self.line:
            self.own_line(distance)
        if 0 <= distance - 1 < self.line:
            self.a_line(distance - 1)
        if 0 <= distance - 2 < self.line:
            self.b_lines(distance - 2)

    def steps(self):
        return self.line + 2

    def end(self):
        slot = self.slot(self.me(), self.place)
        pltpu.make_async_copy(self.shard, self.full.at[slot], self.local_sem).wait()

        @pl.when(self.place + 1 < self.line)
        def _():
            self.copy(slot, 0, self.up(), True).wait_send()

        @pl.when(self.place > 0)
        def _():
            self.copy(slot, 1, self.down(), True).wait_send()

        self.copy(slot, 2, self.a_dev, True).wait_send()
        self.copy(slot, 3, self.b_dev, True).wait_send()
        self.copy(slot, 4, self.core_dev, True).wait_send()
        for distance in range(self.line):
            if distance:
                self.own_line(distance, True)
            self.a_line(distance, True)
            self.b_lines(distance, True)
        partner = self.core_dev[0]
        for place in range(self.line):
            for base in (
                (partner, self.seq), (partner, flip(self.seq, 1)),
                (flip(partner, 2), self.seq), (flip(partner, 2), flip(self.seq, 1)),
            ):
                slot = self.slot(base, place)
                self.copy(slot, 4, self.core_dev).wait_recv()


def relay_scratch(n_dev):
    return [
        pltpu.SemaphoreType.DMA,
        pltpu.SemaphoreType.DMA((n_dev,)),
        pltpu.SemaphoreType.DMA((5, n_dev)),
    ]


def swap(n_seq, send_of, land_of, send_sem, recv_sem):
    grp, seq = lax.axis_index("grp"), lax.axis_index("seq")
    moves = []
    for k in range(1, n_seq):
        to = lax.rem(seq + k, n_seq)
        moves.append(
            pltpu.make_async_remote_copy(
                src_ref=send_of(to),
                dst_ref=land_of(seq),
                send_sem=send_sem.at[k],
                recv_sem=recv_sem.at[k],
                device_id=(grp, to),
                device_id_type=MESH,
            )
        )
    for move in moves:
        move.start()
    return moves


def vision_kernel(
    n_seq, slots,
    patches, piece_col, piece_row, vit_gain, vit_qkv, vit_out, merge_gain, merge_up, merge_down,
    code, want, row_base, attn_qkv,
    table, qkv_all,
    up_v, down_v, normed_s, gathered, hidden, stage, landed,
    load_sem, send1, recv1, send2, recv2, send3, recv3, *relay_sems,
):
    seq = lax.axis_index("seq")
    grp = lax.axis_index("grp")
    up_copy = pltpu.make_async_copy(merge_up, up_v, load_sem.at[0])
    down_copy = pltpu.make_async_copy(merge_down, down_v, load_sem.at[1])
    up_copy.start()
    down_copy.start()
    greet(n_seq, (flip(grp, 1), flip(grp, 2)))
    relay = Relay(n_seq, attn_qkv, qkv_all, *relay_sems)
    relay.begin()

    rows, features = patches.shape
    head_dim = features // VHEADS
    residual = patches[...].astype(jnp.float32)
    normed = rms_scale(residual, vit_gain[...]).astype(jnp.bfloat16)
    projected = jnp.dot(normed, vit_qkv[...], preferred_element_type=jnp.float32)
    q = projected[:, :features].astype(jnp.bfloat16).astype(jnp.float32)
    keys = projected[:, features : 2 * features].astype(jnp.bfloat16)
    values = projected[:, 2 * features :].astype(jnp.bfloat16)
    lane = lax.broadcasted_iota(jnp.int32, (rows, features), 1)
    inside = [(lane >= h * head_dim) & (lane < (h + 1) * head_dim) for h in range(VHEADS)]
    stacked = jnp.concatenate(
        [jnp.where(inside[h], q, 0.0).astype(jnp.bfloat16) for h in range(VHEADS)], axis=0
    )
    scores = lax.dot_general(
        stacked, keys, (((1,), (1,)), ((), ())), preferred_element_type=jnp.float32
    ) * head_dim ** (-0.5)
    scores = scores.reshape(VHEADS, rows, rows)
    allowed = piece_col[...] == piece_row[...]
    scores = jnp.where(allowed[None], scores, -1e30)
    weights = jnp.exp(scores - jnp.max(scores, axis=-1, keepdims=True))
    totals = jnp.sum(weights, axis=-1, keepdims=True)
    mixed = jnp.dot(
        weights.reshape(VHEADS * rows, rows).astype(jnp.bfloat16), values,
        preferred_element_type=jnp.float32,
    )
    top = jnp.zeros((rows, features), jnp.float32)
    low = jnp.ones((rows, features), jnp.float32)
    for h in range(VHEADS):
        top = jnp.where(inside[h], mixed[h * rows : (h + 1) * rows], top)
        low = jnp.where(inside[h], totals[h], low)
    mixture = (top / low).astype(jnp.bfloat16)
    residual = residual + jnp.dot(mixture, vit_out[...], preferred_element_type=jnp.float32)
    merged_in = rms_scale(residual, merge_gain[...])
    own = rows // 4
    chunks = features // LANES
    for j in range(chunks):
        normed_s[j] = merged_in[:, j * LANES : (j + 1) * LANES]
    for part in range(4):
        for j in range(chunks):
            start = part * features + j * LANES
            gathered[seq, :, start : start + LANES] = normed_s[
                j, pl.ds(part, own, stride=4), :
            ].astype(jnp.bfloat16)
    gathered[seq, :, 4 * features :] = code[...]
    moves1 = swap(n_seq, lambda to: gathered.at[seq], lambda me: gathered.at[me], send1, recv1)
    relay.step(1)
    up_copy.wait()
    for move in moves1:
        move.wait_recv()
    all_rows = n_seq * own
    entry = gathered[:, :, : 4 * features].reshape(all_rows, 4 * features)
    pre = jnp.dot(entry, up_v[...], preferred_element_type=jnp.float32)
    hidden[seq] = (0.5 * pre * (1.0 + lax.erf(pre * 0.5**0.5))).astype(jnp.bfloat16)
    moves2 = swap(n_seq, lambda to: hidden.at[seq], lambda me: hidden.at[me], send2, recv2)
    relay.step(2)
    down_copy.wait()
    part_width = hidden.shape[2]

    def term(source):
        start = pl.multiple_of(source * part_width, 32)
        return jnp.dot(
            hidden[source], down_v[pl.ds(start, part_width), :], preferred_element_type=jnp.float32
        )

    codes = gathered[:, :, 4 * features :].reshape(all_rows, LANES).astype(jnp.float32)[:, :1]
    select = jnp.where(codes + row_base[...] == want[...], 1.0, 0.0)
    select = jnp.transpose(select).astype(jnp.bfloat16)
    total = term(seq)
    for k in range(1, n_seq):
        moves2[k - 1].wait_recv()
        total = total + term(lax.rem(seq - k + n_seq, n_seq))
    outgoing = jnp.dot(
        select, total.astype(jnp.bfloat16), preferred_element_type=jnp.float32
    ).astype(jnp.bfloat16)
    stage[...] = outgoing.reshape(stage.shape)
    landed[seq] = stage[seq]
    moves3 = swap(n_seq, lambda to: stage.at[to], lambda me: landed.at[me], send3, recv3)
    for distance in range(3, relay.steps()):
        relay.step(distance)
    for move in moves3:
        move.wait_recv()
    width = landed.shape[2]
    for source in range(n_seq):
        table[:, source * width : (source + 1) * width] = landed[source]
    for moves in (moves1, moves2, moves3):
        for move in moves:
            move.wait_send()
    relay.end()


def attend_kernel(
    n_seq, reach, heads,
    queries, own_kv, positions, starts, attn_out,
    attended, out_all,
    kv, load_sem, send_sem, recv_sem, *relay_sems,
):
    grp, seq = lax.axis_index("grp"), lax.axis_index("seq")
    rows, width = own_kv.shape
    head_dim = width // 2
    greet(n_seq, (flip(grp, 1), flip(grp, 2)))
    moves = []
    for k in range(1, reach + 1):
        moves.append(
            pltpu.make_async_remote_copy(
                src_ref=own_kv,
                dst_ref=kv.at[reach - k],
                send_sem=send_sem.at[k],
                recv_sem=recv_sem.at[k],
                device_id=(grp, lax.rem(seq + k, n_seq)),
                device_id_type=MESH,
            )
        )
    for move in moves:
        move.start()
    relay = Relay(n_seq, attn_out, out_all, *relay_sems)
    relay.begin()
    kv[reach] = own_kv[...]
    for move in moves:
        move.wait_recv()
    span = (reach + 1) * rows
    everything = kv[...].reshape(span, width)
    keys, values = everything[:, :head_dim], everything[:, head_dim:]
    key_pos = (seq - reach) * rows + lax.broadcasted_iota(jnp.int32, (rows, span), 1)
    allowed = (key_pos >= starts[...]) & (key_pos <= positions[...])
    for distance in range(relay.steps()):
        relay.step(distance)
        for h in range(heads) if distance == 1 else ():
            scores = lax.dot_general(
                queries[:, h * head_dim : (h + 1) * head_dim], keys,
                (((1,), (1,)), ((), ())), preferred_element_type=jnp.float32,
            ) * head_dim ** (-0.5)
            scores = jnp.where(allowed, scores, -1e30)
            weights = jnp.exp(scores - jnp.max(scores, axis=-1, keepdims=True))
            totals = jnp.sum(weights, axis=-1, keepdims=True)
            mixed = jnp.dot(
                weights.astype(jnp.bfloat16), values, preferred_element_type=jnp.float32
            )
            attended[:, h * head_dim : (h + 1) * head_dim] = (mixed / totals).astype(jnp.bfloat16)
    for move in moves:
        move.wait_send()
    relay.end()


def out_kernel(attended, weight, layer_in, result):
    width = weight.shape[2]
    for i in range(weight.shape[0]):
        columns = slice(i * width, (i + 1) * width)
        update = jnp.dot(attended[...], weight[i], preferred_element_type=jnp.float32)
        result[:, columns] = (layer_in[:, columns].astype(jnp.float32) + update).astype(jnp.bfloat16)


VMEM = pl.BlockSpec(memory_space=pltpu.VMEM)
ANY = pl.BlockSpec(memory_space=pl.ANY)


def on_device(
    patches, piece_ids, vit_gain, vit_qkv, vit_out, merge_gain, merge_up, merge_down, dest,
    tokens, image_index, doc_lengths, attn_gain, attn_qkv, attn_out,
):
    rows, features = patches.shape
    n_seq, n_grp = lax.axis_size("seq"), lax.axis_size("grp")
    n_dev = n_seq * n_grp
    seq_index = lax.axis_index("seq")
    own = rows // 4
    all_rows = n_seq * own
    capacity = own // (n_seq // 2)
    slots = n_seq * capacity
    bf16, f32 = jnp.bfloat16, jnp.float32

    windows = jnp.arange(rows, dtype=jnp.int32) // WIN
    pieces = piece_ids.reshape(-1) + windows * WIN
    code = dest * capacity + slot_numbers(dest).astype(jnp.int32)
    code = jnp.broadcast_to(code[:, None], (own, LANES)).astype(bf16)
    column = jnp.arange(n_seq * slots, dtype=jnp.int32)
    target, place = column // slots, column % slots
    want = (place // capacity) * (n_seq * capacity) + target * capacity + place % capacity
    row_base = (jnp.arange(all_rows, dtype=jnp.int32) // own) * (n_seq * capacity)

    up_width, down_width = merge_up.shape[1], merge_down.shape[1]
    table, qkv_all = pl.pallas_call(
        functools.partial(vision_kernel, n_seq, slots),
        out_shape=(
            jax.ShapeDtypeStruct((slots, n_seq * down_width), bf16),
            jax.ShapeDtypeStruct((n_dev,) + attn_qkv.shape, bf16),
        ),
        in_specs=[VMEM] * 7 + [ANY] * 2 + [VMEM] * 4,
        out_specs=(VMEM, ANY),
        scratch_shapes=[
            pltpu.VMEM(merge_up.shape, bf16),
            pltpu.VMEM(merge_down.shape, bf16),
            pltpu.VMEM((features // LANES, rows, LANES), f32),
            pltpu.VMEM((n_seq, own, 4 * features + LANES), bf16),
            pltpu.VMEM((n_seq, all_rows, up_width), bf16),
            pltpu.VMEM((n_seq, slots, down_width), bf16),
            pltpu.VMEM((n_seq, slots, down_width), bf16),
            pltpu.SemaphoreType.DMA((2,)),
        ] + [pltpu.SemaphoreType.DMA((n_seq,))] * 6 + relay_scratch(n_dev),
        compiler_params=pltpu.CompilerParams(
            collective_id=0, has_side_effects=True, vmem_limit_bytes=66000000
        ),
    )(
        patches, pieces[:, None], pieces[None, :], vit_gain[None], vit_qkv, vit_out,
        merge_gain[None], merge_up, merge_down, code, want.astype(f32)[None],
        row_base.astype(f32)[:, None], attn_qkv,
    )

    slot_all = jnp.arange(slots, dtype=jnp.int32)
    picker = (image_index[:, None] == slot_all[None, :]).astype(bf16)
    pictured = jnp.dot(picker, table, preferred_element_type=f32).astype(bf16)
    layer_in = jnp.where((image_index < slots)[:, None], pictured, tokens)
    tok_rows = tokens.shape[0]
    normed = rms_scale(layer_in.astype(f32), attn_gain).astype(bf16)
    projected = jnp.dot(
        normed, qkv_all.reshape(-1, attn_qkv.shape[1]), preferred_element_type=f32
    ).astype(bf16)
    query_width = attn_out.shape[0]
    queries = projected[:, :query_width]
    key_value = projected[:, query_width:]
    head_dim = key_value.shape[1] // 2
    head_count = query_width // head_dim
    positions = seq_index * tok_rows + jnp.arange(tok_rows, dtype=jnp.int32)
    lengths = doc_lengths[0]
    starts = jnp.cumsum(lengths) - lengths
    doc_start = jnp.max(
        jnp.where(starts[None, :] <= positions[:, None], starts[None, :], 0), axis=1
    )
    reach = n_seq // 2
    attended, out_all = pl.pallas_call(
        functools.partial(attend_kernel, n_seq, reach, head_count),
        out_shape=(
            jax.ShapeDtypeStruct((tok_rows, query_width), bf16),
            jax.ShapeDtypeStruct((n_dev,) + attn_out.shape, bf16),
        ),
        in_specs=[VMEM] * 5,
        out_specs=(VMEM, ANY),
        scratch_shapes=[
            pltpu.VMEM((reach + 1, tok_rows, 2 * head_dim), bf16),
            pltpu.SemaphoreType.DMA((2,)),
            pltpu.SemaphoreType.DMA((reach + 1,)),
            pltpu.SemaphoreType.DMA((reach + 1,)),
        ] + relay_scratch(n_dev),
        compiler_params=pltpu.CompilerParams(
            collective_id=1, has_side_effects=True, vmem_limit_bytes=60000000
        ),
    )(queries, key_value, positions[:, None], doc_start[:, None], attn_out)

    step = n_dev // 8
    wide = step * attn_out.shape[1]
    return pl.pallas_call(
        out_kernel,
        grid=(n_dev // step,),
        out_shape=jax.ShapeDtypeStruct(tokens.shape, bf16),
        in_specs=[
            pl.BlockSpec((tok_rows, query_width), lambda i: (0, 0)),
            pl.BlockSpec((step,) + attn_out.shape, lambda i: (i, 0, 0)),
            pl.BlockSpec((tok_rows, wide), lambda i: (0, i)),
        ],
        out_specs=pl.BlockSpec((tok_rows, wide), lambda i: (0, i)),
    )(attended, out_all, layer_in)


def solution(mesh):
    placed = (
        P(("grp", "seq"), None),
        P(("grp", "seq"), None),
        P(),
        P(),
        P(),
        P(),
        P(None, "seq"),
        P(None, "seq"),
        P(("grp", "seq")),
        P(("grp", "seq"), None),
        P(("grp", "seq")),
        P("grp", None),
        P(),
        P(("grp", "seq"), None),
        P(None, ("grp", "seq")),
    )
    return jax.shard_map(
        on_device, mesh=mesh, in_specs=placed, out_specs=P(("grp", "seq"), None), check_vma=False
    )
```
